32 devices in a mesh: ctx: 8 (over y, x, core), rec: 4 (over z).
Axes of the slice: x: 2, y: 2, z: 4, core: 2. Of those that a mesh axis runs over, the one named last changes fastest.
Arguments:
- queries: bfloat16 [4, 1024, 4096], P('rec', 'ctx'), may hold values from -6 to 6
- out_grads: bfloat16 [4, 1024, 4096], P('rec', 'ctx'), may hold values from -6 to 6
- log_sums: float32 [4, 32, 1024], P('rec', None, 'ctx'), may hold values from 1.5 to 4
- deltas: float32 [4, 32, 1024], P('rec', None, 'ctx'), may hold values from -6 to 6
- keys: bfloat16 [1024, 256], P('ctx'), may hold values from -6 to 6
- values: bfloat16 [1024, 256], P('ctx'), may hold values from -0.5 to 0.5
- doc_ids: int32 [4, 8], P('rec'), may hold values from 0 to 3, never falling along the last dimension, each value on 1 to 4 neighbouring positions
Outputs:
- query_grads: bfloat16 [4, 1024, 4096], P('rec', 'ctx')
- key_grads: bfloat16 [1024, 256], P(('ctx', 'rec'))
- value_grads: bfloat16 [1024, 256], P(('ctx', 'rec'))
The draws below stay inside these ranges and needn't reach their ends.
Inputs may be any that keep to these rules, and one draw needn't show every extreme that they name: `doc_ids`: in each row the numbers never fall, start at 0, each document spans 1 to 4 blocks and some document spans exactly 4 blocks.
All inputs are finite; a program needn't handle non-finite values.
Results may differ from the reference program's by a relative error of at most 0.0062.
Values may be sent and summed in bfloat16 or wider, within the bound.
A program may use at most 64 MiB of HBM per device.

```python
import math
import jax
import jax.numpy as jnp
import numpy as np
from jax import lax

QH = 32
KVH = 2
HD = 128
TOK = 128
MAXSPAN = 4
NBLK = 8
REC = 4
TOKENS = 1024


def block_scale(key, dims, pieces, low, top_value):
    factor_of, own = 1.0, jax.random.fold_in(key, 6)
    for position, shards_of in pieces:
        heights = jnp.exp(jax.random.uniform(jax.random.fold_in(own, position), (shards_of,), jnp.float32, low / len(pieces), top_value / len(pieces)))
        factor_of = factor_of * jnp.repeat(heights, dims[position] // shards_of).reshape([-1 if axis == position else 1 for axis in range(len(dims))])
    return factor_of


def split_up(amount, total, limit, skew):
    loads = [(1 << 20) // math.isqrt(rank ** skew) + 1 for rank in range(2, amount + 1)]
    spare, holding = total - limit - (amount - 1), [1] * (amount - 1)
    while spare > 0:
        free = [i for i in range(amount - 1) if holding[i] < limit]
        pool, budget = sum([loads[i] for i in free]), spare
        for i in free:
            addition = min(limit - holding[i], max(1, budget * loads[i] // pool), spare)
            holding[i] = holding[i] + addition
            spare = spare - addition
    return np.array([limit] + holding)


def ragged_sizes(stream_key, count, total, bound, slope):
    if count == 2:
        one = jax.random.randint(stream_key, (), max(1, total - bound), min(bound, total - 1) + 1)
        return jnp.stack([one, total - one])
    lengths = jnp.asarray(split_up(count, total, bound, slope), jnp.int32)
    couples = (count - 1) // 2
    donor, taker = lengths[1:1 + 2 * couples:2], lengths[2:2 + 2 * couples:2]
    slack = jnp.minimum(donor - 1, bound - taker)
    shifted = jax.random.randint(jax.random.fold_in(stream_key, 1), (couples,), 0, 1 << 20) % (slack + 1)
    lengths = lengths.at[1:1 + 2 * couples:2].set(donor - shifted).at[2:2 + 2 * couples:2].set(taker + shifted)
    return lengths[jax.random.permutation(jax.random.fold_in(stream_key, 2), count)]


def normal_values(key, extent, scale, most, pieces=(), kind=jnp.bfloat16):
    result = jax.random.normal(key, extent, jnp.float32) * scale
    if len(pieces) > 0:
        result = block_scale(key, extent, pieces, -0.22, 0.18) * result
    return jnp.clip(result, min=-most, max=most).astype(kind)


def setup_inputs(seed: int = 0) -> dict:
    arg_keys = jax.random.split(jax.random.key(seed), 8)
    queries = normal_values(arg_keys[0], (REC, TOKENS, QH * HD), 1.0, 6.0, ((0, 4), (1, 8)))
    out_grads = normal_values(arg_keys[1], (REC, TOKENS, QH * HD), 1.0, 6.0, ((0, 4), (1, 8)))
    log_sums = jnp.clip(1.5 + 2.5 * jax.random.uniform(arg_keys[2], (REC, QH, TOKENS), jnp.float32) ** block_scale(arg_keys[2], (REC, QH, TOKENS), ((0, 4), (2, 8)), -0.2, 0.2), 1.5, 4.0)
    deltas = normal_values(arg_keys[3], (REC, QH, TOKENS), 1.0, 6.0, ((0, 4), (2, 8)), jnp.float32)
    keys = normal_values(arg_keys[4], (TOKENS, KVH * HD), 1.0, 6.0, ((0, 8),))
    values = normal_values(arg_keys[5], (TOKENS, KVH * HD), HD ** -0.5, 0.5, ((0, 8),))
    doc_ids = jax.vmap(lambda own: jnp.searchsorted(jnp.cumsum(ragged_sizes(own, NBLK // 2, NBLK, MAXSPAN, 1)), jnp.arange(NBLK), side="right"))(jax.random.split(arg_keys[6], REC)).reshape((REC, NBLK)).astype(jnp.int32)
    return {"queries": queries, "out_grads": out_grads, "log_sums": log_sums, "deltas": deltas, "keys": keys, "values": values, "doc_ids": doc_ids}


def tile_terms(query_block, grad_block, sums_block, delta_block, key_block, value_block, query_index, key_index):
    rows = query_block.shape[0]
    key_heads = key_block.shape[1] // HD
    group = query_block.shape[1] // (key_heads * HD)
    scale = HD ** -0.5
    query_heads = query_block.astype(jnp.float32).reshape(rows, key_heads, group, HD)
    grad_heads = grad_block.astype(jnp.float32).reshape(rows, key_heads, group, HD)
    key_split = key_block.astype(jnp.float32).reshape(rows, key_heads, HD)
    value_split = value_block.astype(jnp.float32).reshape(rows, key_heads, HD)
    sums_heads = sums_block.reshape(key_heads, group, rows)
    delta_heads = delta_block.reshape(key_heads, group, rows)
    positions = jnp.arange(rows, dtype=jnp.int32)
    query_pos = query_index * rows + positions
    key_pos = key_index * rows + positions
    causal = key_pos[None, :] <= query_pos[:, None]
    scores = jnp.einsum("qkgd,skd->kgqs", query_heads, key_split) * scale
    probs = jnp.where(causal, jnp.exp(scores - sums_heads[..., None]), 0.0)
    dprobs = jnp.einsum("qkgd,skd->kgqs", grad_heads, value_split)
    dscores = probs * (dprobs - delta_heads[..., None])
    probs_b = probs.astype(jnp.bfloat16).astype(jnp.float32)
    dscores_b = dscores.astype(jnp.bfloat16).astype(jnp.float32)
    value_grad = jnp.einsum("kgqs,qkgd->skd", probs_b, grad_heads).reshape(rows, key_heads * HD)
    key_grad = jnp.einsum("kgqs,qkgd->skd", dscores_b, query_heads).reshape(rows, key_heads * HD) * scale
    query_grad = jnp.einsum("kgqs,skd->qkgd", dscores_b, key_split).reshape(rows, -1) * scale
    return query_grad, key_grad, value_grad


def reference(queries, out_grads, log_sums, deltas, keys, values, doc_ids):
    rows = TOK
    span = MAXSPAN
    blocks = NBLK
    width = keys.shape[1]
    qwidth = queries.shape[2]
    pad_rows = (span - 1) * rows
    keys_pad = jnp.concatenate([jnp.zeros((pad_rows, width), keys.dtype), keys], axis=0)
    values_pad = jnp.concatenate([jnp.zeros((pad_rows, width), values.dtype), values], axis=0)
    key_total = jnp.zeros((pad_rows + TOKENS, width), jnp.float32)
    value_total = jnp.zeros((pad_rows + TOKENS, width), jnp.float32)
    order = jnp.arange(blocks, dtype=jnp.int32)
    results = []
    for recur in range(REC):
        ids = doc_ids[recur]
        first = jnp.min(jnp.where(ids[:, None] == ids[None, :], order[None, :], blocks), axis=1).astype(jnp.int32)
        query_all = queries[recur]
        grad_all = out_grads[recur]
        sums_all = log_sums[recur]
        delta_all = deltas[recur]

        def per_block(carry, index):
            key_acc, value_acc = carry
            start = (index * rows).astype(jnp.int32)
            query_block = lax.dynamic_slice_in_dim(query_all, start, rows, 0)
            grad_block = lax.dynamic_slice_in_dim(grad_all, start, rows, 0)
            sums_block = lax.dynamic_slice_in_dim(sums_all, start, rows, 1)
            delta_block = lax.dynamic_slice_in_dim(delta_all, start, rows, 1)
            query_grad = jnp.zeros((rows, qwidth), jnp.float32)
            for back in range(span):
                other = index - back
                kstart = ((other + span - 1) * rows).astype(jnp.int32)
                key_block = lax.dynamic_slice_in_dim(keys_pad, kstart, rows, 0)
                value_block = lax.dynamic_slice_in_dim(values_pad, kstart, rows, 0)
                active = other >= first[index]

                def compute():
                    return tile_terms(query_block, grad_block, sums_block, delta_block, key_block, value_block, index, other)

                def nothing():
                    return (jnp.zeros((rows, qwidth), jnp.float32), jnp.zeros((rows, width), jnp.float32), jnp.zeros((rows, width), jnp.float32))

                terms = lax.cond(active, compute, nothing)
                query_grad = query_grad + terms[0]
                key_acc = lax.dynamic_update_slice_in_dim(key_acc, lax.dynamic_slice_in_dim(key_acc, kstart, rows, 0) + terms[1], kstart, 0)
                value_acc = lax.dynamic_update_slice_in_dim(value_acc, lax.dynamic_slice_in_dim(value_acc, kstart, rows, 0) + terms[2], kstart, 0)
            return (key_acc, value_acc), query_grad.astype(jnp.bfloat16)

        (key_total, value_total), grads = lax.scan(per_block, (key_total, value_total), order)
        results.append(grads.reshape(TOKENS, qwidth))
    query_grads = jnp.stack(results, axis=0)
    return query_grads, key_total[pad_rows:].astype(jnp.bfloat16), value_total[pad_rows:].astype(jnp.bfloat16)
```

```python
import functools
import math

import jax
import jax.numpy as jnp
from jax import lax
from jax.experimental import pallas as pl
from jax.experimental.pallas import tpu as pltpu
from jax.sharding import PartitionSpec as P

HD = 128
MAXSPAN = 4
HEADS = 4
BACK = MAXSPAN - 1
MESH = pl.DeviceIdType.MESH
FAR = 1e30


def kernel(
    q_hbm, g_hbm, sums_ref, delta_ref, k_hbm, v_hbm, ids_ref,
    dq_hbm, dk_ref, dv_ref,
    q_buf, g_buf, kv, key_t, ds_buf, dq_buf, acc, part, landed, total, r_send, r_land,
    load_sem, own_sem, kv_send, kv_recv, g_send, g_recv, rec_send, rec_recv, out_sem,
):
    peers = lax.axis_size("ctx")
    recs = lax.axis_size("rec")
    mine = lax.axis_index("ctx")
    rec = lax.axis_index("rec")
    rows = q_buf.shape[0]
    key_heads = kv.shape[0]
    group = q_buf.shape[1] // (key_heads * HD)
    chunks = group // HEADS
    wide = HEADS * HD
    scale = HD ** (-0.5)
    fold = scale * math.log2(math.e)
    share = rows // recs

    def own_copy(g, which):
        source = (k_hbm, v_hbm)[which]
        return pltpu.make_async_copy(
            source.at[:, pl.ds(g * HD, HD)],
            kv.at[g, which, pl.ds(0, rows), :],
            own_sem.at[g, which],
        )

    def lanes(g, c):
        return pl.ds(pl.multiple_of((g * chunks + c) * wide, wide), wide)

    def load(g, c, which):
        source, target = ((q_hbm, q_buf), (g_hbm, g_buf))[which]
        return pltpu.make_async_copy(
            source.at[0, :, lanes(g, c)], target.at[:, lanes(g, c)], load_sem.at[g, c, which]
        )

    def kv_copy(g, k):
        return pltpu.make_async_remote_copy(
            src_ref=kv.at[g, :, pl.ds(0, rows), :],
            dst_ref=kv.at[g, :, pl.ds(k * rows, rows), :],
            send_sem=kv_send.at[g, k - 1],
            recv_sem=kv_recv.at[g, k - 1],
            device_id={"ctx": lax.rem(mine + k, peers)},
            device_id_type=MESH,
        )

    def grad_copy(g, k):
        return pltpu.make_async_remote_copy(
            src_ref=part.at[g, k - 1],
            dst_ref=landed.at[g, k - 1],
            send_sem=g_send.at[g, k - 1],
            recv_sem=g_recv.at[g, k - 1],
            device_id={"ctx": lax.rem(mine - k + peers, peers)},
            device_id_type=MESH,
        )

    def rec_copy(g, j):
        target = lax.rem(rec + j, recs)
        return pltpu.make_async_remote_copy(
            src_ref=r_send.at[g, :, pl.ds(pl.multiple_of(target * share, share), share), :],
            dst_ref=r_land.at[g, j - 1],
            send_sem=rec_send.at[g, j - 1],
            recv_sem=rec_recv.at[g, j - 1],
            device_id={"rec": target},
            device_id_type=MESH,
        )

    for g in range(key_heads):
        for which in range(2):
            own_copy(g, which).start()
    for g in range(key_heads):
        for c in range(chunks):
            for which in range(2):
                load(g, c, which).start()

    barrier = pltpu.get_barrier_semaphore()
    for k in range(1, MAXSPAN):
        for other in (lax.rem(mine + k, peers), lax.rem(mine - k + peers, peers)):
            pl.semaphore_signal(barrier, inc=1, device_id={"ctx": other}, device_id_type=MESH)
    for j in range(1, recs):
        pl.semaphore_signal(
            barrier, inc=1, device_id={"rec": lax.rem(rec + j, recs)}, device_id_type=MESH
        )
    for k in range(1, MAXSPAN):
        @pl.when(mine < k)
        def _():
            kv[:, :, pl.ds(k * rows, rows), :] = jnp.zeros((key_heads, 2, rows, HD), kv.dtype)

        @pl.when(mine + k >= peers)
        def _():
            landed[:, k - 1] = jnp.zeros((key_heads, 2, rows, HD), landed.dtype)
    acc[...] = jnp.zeros_like(acc)
    pl.semaphore_wait(barrier, 2 * BACK + recs - 1)

    for g in range(key_heads):
        for which in range(2):
            own_copy(g, which).wait()
        for k in range(1, MAXSPAN):
            @pl.when(mine + k < peers)
            def _():
                kv_copy(g, k).start()

    here = ids_ref[0, mine]
    far = [jnp.float32(0.0)]
    for k in range(1, MAXSPAN):
        same = (ids_ref[0, jnp.maximum(mine - k, 0)] == here) & (mine >= k)
        far.append(jnp.where(same, 0.0, FAR).astype(jnp.float32))

    def heads_down(ref, g, c):
        first = (g * chunks + c) * HEADS
        return jnp.concatenate(
            [ref[:, pl.ds(pl.multiple_of((first + i) * HD, HD), HD)] for i in range(HEADS)], axis=0
        )

    def heads_along(ref, g, c):
        first = (g * chunks + c) * HEADS
        return jnp.concatenate([ref[0, pl.ds(first + i, 1), :] for i in range(HEADS)], axis=1)

    inner = (((1,), (1,)), ((), ()))

    def sweep(g, tiles, loads, finish):
        @pl.loop(0, chunks)
        def _(c):
            if loads:
                for which in range(2):
                    load(g, c, which).wait()
            query = heads_down(q_buf, g, c)
            grad = heads_down(g_buf, g, c)
            sums = heads_along(sums_ref, g, c) * math.log2(math.e)
            delta = heads_along(delta_ref, g, c)
            for k in tiles:
                at = pl.ds(k * rows, rows)
                scores = lax.dot_general(
                    kv[g, 0, at, :], query, inner, preferred_element_type=jnp.float32
                )
                dprobs = lax.dot_general(
                    kv[g, 1, at, :], grad, inner, preferred_element_type=jnp.float32
                )
                probs = jnp.exp2(scores * fold - (sums + far[k]))
                if k == 0:
                    u = lax.broadcasted_iota(jnp.int32, (rows, wide), 0)
                    t = lax.broadcasted_iota(jnp.int32, (rows, wide), 1) & (rows - 1)
                    probs = jnp.where(u <= t, probs, 0.0)
                ds = (probs * (dprobs - delta)).astype(jnp.bfloat16)
                probs = probs.astype(jnp.bfloat16)
                ds_buf[at, lanes(g, c)] = ds
                acc[g, 0, at, :] += jnp.dot(ds, query, preferred_element_type=jnp.float32)
                acc[g, 1, at, :] += jnp.dot(probs, grad, preferred_element_type=jnp.float32)
            if finish:
                dq = jnp.dot(
                    key_t[g], ds_buf[:, lanes(g, c)], preferred_element_type=jnp.float32
                ) * scale
                for i in range(HEADS):
                    at = pl.ds(pl.multiple_of(((g * chunks + c) * HEADS + i) * HD, HD), HD)
                    dq_buf[:, at] = dq[:, i * rows:(i + 1) * rows].T.astype(dq_buf.dtype)
                pltpu.make_async_copy(
                    dq_buf.at[:, lanes(g, c)], dq_hbm.at[0, :, lanes(g, c)], out_sem.at[g, c]
                ).start()

    def turn(g, k):
        at = pl.ds(k * rows, rows)
        key_t[g, :, k * rows:(k + 1) * rows] = kv[g, 0, at, :].T

    def arrive(g):
        for k in range(1, MAXSPAN):
            @pl.when(mine >= k)
            def _():
                kv_copy(g, k).wait_recv()
            turn(g, k)

    def leave(g):
        for k in range(1, MAXSPAN):
            part[g, k - 1] = acc[g, :, k * rows:(k + 1) * rows, :].astype(part.dtype)

            @pl.when(mine >= k)
            def _():
                grad_copy(g, k).start()

    def across(g):
        whole = acc[g, :, 0:rows, :]
        for k in range(1, MAXSPAN):
            @pl.when(mine + k < peers)
            def _():
                grad_copy(g, k).wait_recv()
        for k in range(1, MAXSPAN):
            whole = whole + landed[g, k - 1].astype(jnp.float32)
        total[g] = whole
        r_send[g] = whole.astype(r_send.dtype)
        for j in range(1, recs):
            rec_copy(g, j).start()

    def close(g):
        whole = total[g, :, pl.ds(pl.multiple_of(rec * share, share), share), :]
        for j in range(1, recs):
            rec_copy(g, j).wait_recv()
            whole = whole + r_land[g, j - 1].astype(jnp.float32)
        dk_ref[:, g * HD:(g + 1) * HD] = (whole[0] * scale).astype(dk_ref.dtype)
        dv_ref[:, g * HD:(g + 1) * HD] = whole[1].astype(dv_ref.dtype)

    off = tuple(range(1, MAXSPAN))
    last = key_heads - 1
    for g in range(key_heads):
        turn(g, 0)
    for g in range(last):
        sweep(g, (0,), True, False)
    for g in range(last):
        arrive(g)
        sweep(g, off, False, True)
        leave(g)
    arrive(last)
    sweep(last, off, True, False)
    leave(last)
    for g in range(last):
        across(g)
    sweep(last, (0,), False, True)
    across(last)
    for g in range(key_heads):
        close(g)
    for g in range(key_heads):
        for c in range(chunks):
            pltpu.make_async_copy(
                dq_buf.at[:, lanes(g, c)], dq_hbm.at[0, :, lanes(g, c)], out_sem.at[g, c]
            ).wait()
        for k in range(1, MAXSPAN):
            @pl.when(mine + k < peers)
            def _():
                kv_copy(g, k).wait_send()

            @pl.when(mine >= k)
            def _():
                grad_copy(g, k).wait_send()
        for j in range(1, recs):
            rec_copy(g, j).wait_send()


def per_device(queries, out_grads, log_sums, deltas, keys, values, doc_ids):
    recs = lax.axis_size("rec")
    rows, width = queries.shape[1:]
    key_heads = keys.shape[1] // HD
    chunks = width // (key_heads * HD * HEADS)
    span = MAXSPAN * rows
    half = jnp.bfloat16
    dma = pltpu.SemaphoreType.DMA
    anywhere = pl.BlockSpec(memory_space=pl.ANY)
    vmem = pl.BlockSpec(memory_space=pltpu.VMEM)
    return pl.pallas_call(
        kernel,
        out_shape=(
            jax.ShapeDtypeStruct(queries.shape, half),
            jax.ShapeDtypeStruct((rows // recs, keys.shape[1]), half),
            jax.ShapeDtypeStruct((rows // recs, keys.shape[1]), half),
        ),
        in_specs=[
            anywhere, anywhere, vmem, vmem, anywhere, anywhere,
            pl.BlockSpec(memory_space=pltpu.SMEM),
        ],
        out_specs=(anywhere, vmem, vmem),
        scratch_shapes=[
            pltpu.VMEM((rows, width), half),
            pltpu.VMEM((rows, width), half),
            pltpu.VMEM((key_heads, 2, span, HD), half),
            pltpu.VMEM((key_heads, HD, span), half),
            pltpu.VMEM((span, width), half),
            pltpu.VMEM((rows, width), half),
            pltpu.VMEM((key_heads, 2, span, HD), jnp.float32),
            pltpu.VMEM((key_heads, BACK, 2, rows, HD), half),
            pltpu.VMEM((key_heads, BACK, 2, rows, HD), half),
            pltpu.VMEM((key_heads, 2, rows, HD), jnp.float32),
            pltpu.VMEM((key_heads, 2, rows, HD), half),
            pltpu.VMEM((key_heads, max(recs - 1, 1), 2, rows // recs, HD), half),
            dma((key_heads, chunks, 2)),
            dma((key_heads, 2)),
            dma((key_heads, BACK)),
            dma((key_heads, BACK)),
            dma((key_heads, BACK)),
            dma((key_heads, BACK)),
            dma((key_heads, max(recs - 1, 1))),
            dma((key_heads, max(recs - 1, 1))),
            dma((key_heads, chunks)),
        ],
        compiler_params=pltpu.CompilerParams(
            collective_id=0, has_side_effects=True, vmem_limit_bytes=48 * 1024 * 1024
        ),
    )(queries, out_grads, log_sums, deltas, keys, values, doc_ids)


def solution(mesh):
    return jax.shard_map(
        per_device,
        mesh=mesh,
        in_specs=(
            P("rec", "ctx", None),
            P("rec", "ctx", None),
            P("rec", None, "ctx"),
            P("rec", None, "ctx"),
            P("ctx", None),
            P("ctx", None),
            P("rec", None),
        ),
        out_specs=(P("rec", "ctx", None), P(("ctx", "rec"), None), P(("ctx", "rec"), None)),
        check_vma=False,
    )
```

```python
import functools
import math

import jax
import jax.numpy as jnp
from jax import lax
from jax.experimental import pallas as pl
from jax.experimental.pallas import tpu as pltpu
from jax.sharding import PartitionSpec as P

HD = 128
MAXSPAN = 4
HEADS = 4
BACK = MAXSPAN - 1
MESH = pl.DeviceIdType.MESH
FAR = 1e30


def kernel(
    q_hbm, g_hbm, sums_hbm, delta_hbm, k_hbm, v_hbm, ids_hbm,
    dq_hbm, dk_ref, dv_ref,
    q_buf, g_buf, sums_ref, delta_ref, ids_ref, kv, key_t, ds_buf, dq_buf, acc, part, landed, total, r_send, r_land,
    load_sem, own_sem, small_sem, kv_send, kv_recv, g_send, g_recv, rec_send, rec_recv, out_sem,
):
    peers = lax.axis_size("ctx")
    recs = lax.axis_size("rec")
    mine = lax.axis_index("ctx")
    rec = lax.axis_index("rec")
    rows = q_buf.shape[0]
    key_heads = kv.shape[0]
    group = q_buf.shape[1] // (key_heads * HD)
    chunks = group // HEADS
    wide = HEADS * HD
    scale = HD ** (-0.5)
    fold = scale * math.log2(math.e)
    share = rows // recs

    def own_copy(g, which):
        source = (k_hbm, v_hbm)[which]
        return pltpu.make_async_copy(
            source.at[:, pl.ds(g * HD, HD)],
            kv.at[g, which, pl.ds(0, rows), :],
            own_sem.at[g, which],
        )

    def lanes(g, c):
        return pl.ds(pl.multiple_of((g * chunks + c) * wide, wide), wide)

    def load(g, c, which):
        source, target = ((q_hbm, q_buf), (g_hbm, g_buf))[which]
        return pltpu.make_async_copy(
            source.at[0, :, lanes(g, c)], target.at[:, lanes(g, c)], load_sem.at[g, c, which]
        )

    def out_copy(g, c):
        return pltpu.make_async_copy(
            dq_buf.at[:, lanes(g, c)], dq_hbm.at[0, :, lanes(g, c)], out_sem.at[g, c]
        )

    def kv_copy(g, k):
        return pltpu.make_async_remote_copy(
            src_ref=kv.at[g, :, pl.ds(0, rows), :],
            dst_ref=kv.at[g, :, pl.ds(k * rows, rows), :],
            send_sem=kv_send.at[g, k - 1],
            recv_sem=kv_recv.at[g, k - 1],
            device_id={"ctx": lax.rem(mine + k, peers)},
            device_id_type=MESH,
        )

    def grad_copy(g, k):
        return pltpu.make_async_remote_copy(
            src_ref=part.at[g, k - 1],
            dst_ref=landed.at[g, k - 1],
            send_sem=g_send.at[g, k - 1],
            recv_sem=g_recv.at[g, k - 1],
            device_id={"ctx": lax.rem(mine - k + peers, peers)},
            device_id_type=MESH,
        )

    def rec_copy(g, j):
        target = lax.rem(rec + j, recs)
        return pltpu.make_async_remote_copy(
            src_ref=r_send.at[g, :, pl.ds(pl.multiple_of(target * share, share), share), :],
            dst_ref=r_land.at[g, j - 1],
            send_sem=rec_send.at[g, j - 1],
            recv_sem=rec_recv.at[g, j - 1],
            device_id={"rec": target},
            device_id_type=MESH,
        )

    for g in range(key_heads):
        for which in range(2):
            own_copy(g, which).start()
    small = [
        pltpu.make_async_copy(source, target, small_sem.at[i])
        for i, (source, target) in enumerate(
            ((sums_hbm, sums_ref), (delta_hbm, delta_ref), (ids_hbm, ids_ref))
        )
    ]
    for copy in small:
        copy.start()
    for g in range(key_heads):
        for c in range(chunks):
            for which in range(2):
                load(g, c, which).start()

    barrier = pltpu.get_barrier_semaphore()
    for k in range(1, MAXSPAN):
        for other in (lax.rem(mine + k, peers), lax.rem(mine - k + peers, peers)):
            pl.semaphore_signal(barrier, inc=1, device_id={"ctx": other}, device_id_type=MESH)
    for j in range(1, recs):
        pl.semaphore_signal(
            barrier, inc=1, device_id={"rec": lax.rem(rec + j, recs)}, device_id_type=MESH
        )
    for k in range(1, MAXSPAN):
        @pl.when(mine < k)
        def _():
            kv[:, :, pl.ds(k * rows, rows), :] = jnp.zeros((key_heads, 2, rows, HD), kv.dtype)

        @pl.when(mine + k >= peers)
        def _():
            landed[:, k - 1] = jnp.zeros((key_heads, 2, rows, HD), landed.dtype)
    acc[...] = jnp.zeros_like(acc)
    pl.semaphore_wait(barrier, 2 * BACK + recs - 1)

    for g in range(key_heads):
        for which in range(2):
            own_copy(g, which).wait()
        for k in range(1, MAXSPAN):
            @pl.when(mine + k < peers)
            def _():
                kv_copy(g, k).start()

    for copy in small:
        copy.wait()
    here = ids_ref[0, mine]
    far = [jnp.float32(0.0)]
    for k in range(1, MAXSPAN):
        same = (ids_ref[0, jnp.maximum(mine - k, 0)] == here) & (mine >= k)
        far.append(jnp.where(same, 0.0, FAR).astype(jnp.float32))

    def heads_down(ref, g, c):
        first = (g * chunks + c) * HEADS
        return jnp.concatenate(
            [ref[:, pl.ds(pl.multiple_of((first + i) * HD, HD), HD)] for i in range(HEADS)], axis=0
        )

    def heads_along(ref, g, c):
        first = (g * chunks + c) * HEADS
        return jnp.concatenate([ref[0, pl.ds(first + i, 1), :] for i in range(HEADS)], axis=1)

    inner = (((1,), (1,)), ((), ()))

    def sweep(g, tiles, loads, finish):
        @pl.loop(0, chunks)
        def _(c):
            if loads:
                for which in range(2):
                    load(g, c, which).wait()
            query = heads_down(q_buf, g, c)
            grad = heads_down(g_buf, g, c)
            sums = heads_along(sums_ref, g, c) * math.log2(math.e)
            delta = heads_along(delta_ref, g, c)
            for k in tiles:
                at = pl.ds(k * rows, rows)
                scores = lax.dot_general(
                    kv[g, 0, at, :], query, inner, preferred_element_type=jnp.float32
                )
                dprobs = lax.dot_general(
                    kv[g, 1, at, :], grad, inner, preferred_element_type=jnp.float32
                )
                probs = jnp.exp2(scores * fold - (sums + far[k]))
                if k == 0:
                    u = lax.broadcasted_iota(jnp.int32, (rows, wide), 0)
                    t = lax.broadcasted_iota(jnp.int32, (rows, wide), 1) & (rows - 1)
                    probs = jnp.where(u <= t, probs, 0.0)
                ds = (probs * (dprobs - delta)).astype(jnp.bfloat16)
                probs = probs.astype(jnp.bfloat16)
                ds_buf[at, lanes(g, c)] = ds
                acc[g, 0, at, :] += jnp.dot(ds, query, preferred_element_type=jnp.float32)
                acc[g, 1, at, :] += jnp.dot(probs, grad, preferred_element_type=jnp.float32)
            if finish:
                dq = jnp.dot(
                    key_t[g], ds_buf[:, lanes(g, c)], preferred_element_type=jnp.float32
                ) * scale
                for i in range(HEADS):
                    at = pl.ds(pl.multiple_of(((g * chunks + c) * HEADS + i) * HD, HD), HD)
                    dq_buf[:, at] = dq[:, i * rows:(i + 1) * rows].T.astype(dq_buf.dtype)
                out_copy(g, c).start()

    def turn(g, k):
        at = pl.ds(k * rows, rows)
        key_t[g, :, k * rows:(k + 1) * rows] = kv[g, 0, at, :].T

    def arrive(g):
        for k in range(1, MAXSPAN):
            @pl.when(mine >= k)
            def _():
                kv_copy(g, k).wait_recv()
            turn(g, k)

    def leave(g):
        for k in range(1, MAXSPAN):
            part[g, k - 1] = acc[g, :, k * rows:(k + 1) * rows, :].astype(part.dtype)

            @pl.when(mine >= k)
            def _():
                grad_copy(g, k).start()

    def across(g):
        whole = acc[g, :, 0:rows, :]
        for k in range(1, MAXSPAN):
            @pl.when(mine + k < peers)
            def _():
                grad_copy(g, k).wait_recv()
        for k in range(1, MAXSPAN):
            whole = whole + landed[g, k - 1].astype(jnp.float32)
        total[g] = whole
        r_send[g] = whole.astype(r_send.dtype)
        for j in range(1, recs):
            rec_copy(g, j).start()

    def close(g):
        whole = total[g, :, pl.ds(pl.multiple_of(rec * share, share), share), :]
        for j in range(1, recs):
            rec_copy(g, j).wait_recv()
            whole = whole + r_land[g, j - 1].astype(jnp.float32)
        dk_ref[:, g * HD:(g + 1) * HD] = (whole[0] * scale).astype(dk_ref.dtype)
        dv_ref[:, g * HD:(g + 1) * HD] = whole[1].astype(dv_ref.dtype)

    off = tuple(range(1, MAXSPAN))
    last = key_heads - 1
    for g in range(key_heads):
        turn(g, 0)
    for g in range(last):
        sweep(g, (0,), True, False)
    for g in range(last):
        arrive(g)
        sweep(g, off, False, True)
        leave(g)
    arrive(last)
    sweep(last, off, True, False)
    leave(last)
    for g in range(last):
        across(g)
    sweep(last, (0,), False, True)
    across(last)
    for g in range(key_heads):
        close(g)
    for g in range(key_heads):
        for c in range(chunks):
            out_copy(g, c).wait()
        for k in range(1, MAXSPAN):
            @pl.when(mine + k < peers)
            def _():
                kv_copy(g, k).wait_send()

            @pl.when(mine >= k)
            def _():
                grad_copy(g, k).wait_send()
        for j in range(1, recs):
            rec_copy(g, j).wait_send()


def per_device(queries, out_grads, log_sums, deltas, keys, values, doc_ids):
    recs = lax.axis_size("rec")
    rows, width = queries.shape[1:]
    key_heads = keys.shape[1] // HD
    chunks = width // (key_heads * HD * HEADS)
    span = MAXSPAN * rows
    half = jnp.bfloat16
    dma = pltpu.SemaphoreType.DMA
    far_off = pl.BlockSpec(memory_space=pltpu.HBM)
    vmem = pl.BlockSpec(memory_space=pltpu.VMEM)
    return pl.pallas_call(
        kernel,
        out_shape=(
            jax.ShapeDtypeStruct(queries.shape, half),
            jax.ShapeDtypeStruct((rows // recs, keys.shape[1]), half),
            jax.ShapeDtypeStruct((rows // recs, keys.shape[1]), half),
        ),
        in_specs=[far_off] * 7,
        out_specs=(far_off, vmem, vmem),
        scratch_shapes=[
            pltpu.VMEM((rows, width), half),
            pltpu.VMEM((rows, width), half),
            pltpu.VMEM(log_sums.shape, jnp.float32),
            pltpu.VMEM(deltas.shape, jnp.float32),
            pltpu.SMEM(doc_ids.shape, jnp.int32),
            pltpu.VMEM((key_heads, 2, span, HD), half),
            pltpu.VMEM((key_heads, HD, span), half),
            pltpu.VMEM((span, width), half),
            pltpu.VMEM((rows, width), half),
            pltpu.VMEM((key_heads, 2, span, HD), jnp.float32),
            pltpu.VMEM((key_heads, BACK, 2, rows, HD), half),
            pltpu.VMEM((key_heads, BACK, 2, rows, HD), half),
            pltpu.VMEM((key_heads, 2, rows, HD), jnp.float32),
            pltpu.VMEM((key_heads, 2, rows, HD), half),
            pltpu.VMEM((key_heads, max(recs - 1, 1), 2, rows // recs, HD), half),
            dma((key_heads, chunks, 2)),
            dma((key_heads, 2)),
            dma((3,)),
            dma((key_heads, BACK)),
            dma((key_heads, BACK)),
            dma((key_heads, BACK)),
            dma((key_heads, BACK)),
            dma((key_heads, max(recs - 1, 1))),
            dma((key_heads, max(recs - 1, 1))),
            dma((key_heads, chunks)),
        ],
        compiler_params=pltpu.CompilerParams(
            collective_id=0, has_side_effects=True, vmem_limit_bytes=67_043_328
        ),
    )(queries, out_grads, log_sums, deltas, keys, values, doc_ids)


def solution(mesh):
    return jax.shard_map(
        per_device,
        mesh=mesh,
        in_specs=(
            P("rec", "ctx", None),
            P("rec", "ctx", None),
            P("rec", None, "ctx"),
            P("rec", None, "ctx"),
            P("ctx", None),
            P("ctx", None),
            P("rec", None),
        ),
        out_specs=(P("rec", "ctx", None), P(("ctx", "rec"), None), P(("ctx", "rec"), None)),
        check_vma=False,
    )
```

```python
import functools
import math

import jax
import jax.numpy as jnp
from jax import lax
from jax.experimental import pallas as pl
from jax.experimental.pallas import tpu as pltpu
from jax.sharding import PartitionSpec as P

HD = 128
MAXSPAN = 4
HEADS = 4
BACK = MAXSPAN - 1
MESH = pl.DeviceIdType.MESH
FAR = 1e30
PIECES = 4


def kernel(
    q_hbm, g_hbm, sums_hbm, delta_hbm, k_hbm, v_hbm, ids_hbm,
    dq_hbm, dk_ref, dv_ref,
    q_buf, g_buf, sums_ref, delta_ref, ids_ref, kv, key_t, ds_buf, dq_buf, acc, part, landed, total, r_send, r_land,
    load_sem, own_sem, small_sem, kv_send, kv_recv, g_send, g_recv, rec_send, rec_recv, out_sem,
):
    peers = lax.axis_size("ctx")
    recs = lax.axis_size("rec")
    mine = lax.axis_index("ctx")
    rec = lax.axis_index("rec")
    rows = q_buf.shape[0]
    key_heads = kv.shape[0]
    group = q_buf.shape[1] // (key_heads * HD)
    chunks = group // HEADS
    wide = HEADS * HD
    scale = HD ** (-0.5)
    fold = scale * math.log2(math.e)
    share = rows // recs

    def own_copy(g, which):
        source = (k_hbm, v_hbm)[which]
        return pltpu.make_async_copy(
            source.at[:, pl.ds(g * HD, HD)],
            kv.at[g, which, pl.ds(0, rows), :],
            own_sem.at[g, which],
        )

    def lanes(g, c):
        return pl.ds(pl.multiple_of((g * chunks + c) * wide, wide), wide)

    def load(g, c, which):
        source, target = ((q_hbm, q_buf), (g_hbm, g_buf))[which]
        return pltpu.make_async_copy(
            source.at[0, :, lanes(g, c)], target.at[:, lanes(g, c)], load_sem.at[g, c, which]
        )

    def out_copy(g, c):
        return pltpu.make_async_copy(
            dq_buf.at[:, lanes(g, c)], dq_hbm.at[0, :, lanes(g, c)], out_sem.at[g, c]
        )

    def kv_copy(g, k):
        return pltpu.make_async_remote_copy(
            src_ref=kv.at[g, :, pl.ds(0, rows), :],
            dst_ref=kv.at[g, :, pl.ds(k * rows, rows), :],
            send_sem=kv_send.at[g, k - 1],
            recv_sem=kv_recv.at[g, k - 1],
            device_id={"ctx": lax.rem(mine + k, peers)},
            device_id_type=MESH,
        )

    def grad_copy(g, k):
        return pltpu.make_async_remote_copy(
            src_ref=part.at[g, k - 1],
            dst_ref=landed.at[g, k - 1],
            send_sem=g_send.at[g, k - 1],
            recv_sem=g_recv.at[g, k - 1],
            device_id={"ctx": lax.rem(mine - k + peers, peers)},
            device_id_type=MESH,
        )

    def rec_copy(g, j):
        target = lax.rem(rec + j, recs)
        return pltpu.make_async_remote_copy(
            src_ref=r_send.at[g, :, pl.ds(pl.multiple_of(target * share, share), share), :],
            dst_ref=r_land.at[g, j - 1],
            send_sem=rec_send.at[g, j - 1],
            recv_sem=rec_recv.at[g, j - 1],
            device_id={"rec": target},
            device_id_type=MESH,
        )

    for g in range(key_heads):
        for which in range(2):
            own_copy(g, which).start()
    small = [
        pltpu.make_async_copy(source, target, small_sem.at[i])
        for i, (source, target) in enumerate(
            ((sums_hbm, sums_ref), (delta_hbm, delta_ref), (ids_hbm, ids_ref))
        )
    ]
    for copy in small:
        copy.start()
    for g in range(key_heads):
        for c in range(chunks):
            for which in range(2):
                load(g, c, which).start()

    barrier = pltpu.get_barrier_semaphore()
    for k in range(1, MAXSPAN):
        for other in (lax.rem(mine + k, peers), lax.rem(mine - k + peers, peers)):
            pl.semaphore_signal(barrier, inc=1, device_id={"ctx": other}, device_id_type=MESH)
    for j in range(1, recs):
        pl.semaphore_signal(
            barrier, inc=1, device_id={"rec": lax.rem(rec + j, recs)}, device_id_type=MESH
        )
    for k in range(1, MAXSPAN):
        @pl.when(mine < k)
        def _():
            kv[:, :, pl.ds(k * rows, rows), :] = jnp.zeros((key_heads, 2, rows, HD), kv.dtype)

        @pl.when(mine + k >= peers)
        def _():
            landed[:, k - 1] = jnp.zeros((key_heads, 2, rows, HD), landed.dtype)
    acc[...] = jnp.zeros_like(acc)
    pl.semaphore_wait(barrier, 2 * BACK + recs - 1)

    for g in range(key_heads):
        for which in range(2):
            own_copy(g, which).wait()
        for k in range(1, MAXSPAN):
            @pl.when(mine + k < peers)
            def _():
                kv_copy(g, k).start()

    for copy in small:
        copy.wait()
    here = ids_ref[0, mine]
    far = [jnp.float32(0.0)]
    for k in range(1, MAXSPAN):
        same = (ids_ref[0, jnp.maximum(mine - k, 0)] == here) & (mine >= k)
        far.append(jnp.where(same, 0.0, FAR).astype(jnp.float32))

    def heads_down(ref, g, c):
        first = (g * chunks + c) * HEADS
        return jnp.concatenate(
            [ref[:, pl.ds(pl.multiple_of((first + i) * HD, HD), HD)] for i in range(HEADS)], axis=0
        )

    def heads_along(ref, g, c):
        first = (g * chunks + c) * HEADS
        return jnp.concatenate([ref[0, pl.ds(first + i, 1), :] for i in range(HEADS)], axis=1)

    inner = (((1,), (1,)), ((), ()))

    def sweep(g, k):
        at = pl.ds(k * rows, rows)

        @pl.loop(0, chunks)
        def _(c):
            if k == 0:
                for which in range(2):
                    load(g, c, which).wait()
            query = heads_down(q_buf, g, c)
            grad = heads_down(g_buf, g, c)
            sums = heads_along(sums_ref, g, c) * math.log2(math.e) + far[k]
            delta = heads_along(delta_ref, g, c)
            scores = lax.dot_general(
                kv[g, 0, at, :], query, inner, preferred_element_type=jnp.float32
            )
            dprobs = lax.dot_general(
                kv[g, 1, at, :], grad, inner, preferred_element_type=jnp.float32
            )
            probs = jnp.exp2(scores * fold - sums)
            if k == 0:
                u = lax.broadcasted_iota(jnp.int32, (rows, wide), 0)
                t = lax.broadcasted_iota(jnp.int32, (rows, wide), 1) & (rows - 1)
                probs = jnp.where(u <= t, probs, 0.0)
            ds = (probs * (dprobs - delta)).astype(jnp.bfloat16)
            probs = probs.astype(jnp.bfloat16)
            ds_buf[at, lanes(g, c)] = ds
            acc[g, 0, at, :] += jnp.dot(ds, query, preferred_element_type=jnp.float32)
            acc[g, 1, at, :] += jnp.dot(probs, grad, preferred_element_type=jnp.float32)

    def query_side(g):
        @pl.loop(0, chunks)
        def _(c):
            dq = jnp.dot(
                key_t[g], ds_buf[:, lanes(g, c)], preferred_element_type=jnp.float32
            ) * scale
            for i in range(HEADS):
                at = pl.ds(pl.multiple_of(((g * chunks + c) * HEADS + i) * HD, HD), HD)
                dq_buf[:, at] = dq[:, i * rows:(i + 1) * rows].T.astype(dq_buf.dtype)
            out_copy(g, c).start()

    def turn(g, k):
        at = pl.ds(k * rows, rows)
        key_t[g, :, k * rows:(k + 1) * rows] = kv[g, 0, at, :].T

    def tile(g, k):
        @pl.when(mine >= k)
        def _():
            kv_copy(g, k).wait_recv()
        sweep(g, k)
        part[g, k - 1] = acc[g, :, k * rows:(k + 1) * rows, :].astype(part.dtype)

        @pl.when(mine >= k)
        def _():
            grad_copy(g, k).start()
        turn(g, k)

    def across(g):
        whole = acc[g, :, 0:rows, :]
        for k in range(1, MAXSPAN):
            @pl.when(mine + k < peers)
            def _():
                grad_copy(g, k).wait_recv()
        for k in range(1, MAXSPAN):
            whole = whole + landed[g, k - 1].astype(jnp.float32)
        total[g] = whole
        r_send[g] = whole.astype(r_send.dtype)
        for j in range(1, recs):
            rec_copy(g, j).start()

    def close(g):
        whole = total[g, :, pl.ds(pl.multiple_of(rec * share, share), share), :]
        for j in range(1, recs):
            rec_copy(g, j).wait_recv()
            whole = whole + r_land[g, j - 1].astype(jnp.float32)
        dk_ref[:, g * HD:(g + 1) * HD] = (whole[0] * scale).astype(dk_ref.dtype)
        dv_ref[:, g * HD:(g + 1) * HD] = whole[1].astype(dv_ref.dtype)

    last = key_heads - 1
    for g in range(key_heads):
        sweep(g, 0)
        turn(g, 0)
    for g in range(key_heads):
        order = range(1, MAXSPAN) if g < last else range(BACK, 0, -1)
        for k in order:
            tile(g, k)
    for g in range(last):
        across(g)
        query_side(g)
    across(last)
    query_side(last)
    for g in range(key_heads):
        close(g)
    for g in range(key_heads):
        for c in range(chunks):
            out_copy(g, c).wait()
        for k in range(1, MAXSPAN):
            @pl.when(mine + k < peers)
            def _():
                kv_copy(g, k).wait_send()

            @pl.when(mine >= k)
            def _():
                grad_copy(g, k).wait_send()
        for j in range(1, recs):
            rec_copy(g, j).wait_send()


def finish(dq_in, dk_in, dv_in, dq_out, dk_out, dv_out, big, dk, dv, into, out):
    pieces = big.shape[0]
    depth = big.shape[1]
    pairs = [
        (dq_in.at[0, pl.ds(i * depth, depth), :], big.at[i], dq_out.at[0, pl.ds(i * depth, depth), :])
        for i in range(pieces)
    ] + [(dk_in, dk, dk_out), (dv_in, dv, dv_out)]
    ins = [pltpu.make_async_copy(p[0], p[1], into.at[i]) for i, p in enumerate(pairs)]
    outs = [pltpu.make_async_copy(p[1], p[2], out.at[i]) for i, p in enumerate(pairs)]
    for copy in ins:
        copy.start()
    for arrived, leaving in zip(ins, outs):
        arrived.wait()
        leaving.start()
    for copy in outs:
        copy.wait()


def per_device(queries, out_grads, log_sums, deltas, keys, values, doc_ids):
    recs = lax.axis_size("rec")
    rows, width = queries.shape[1:]
    key_heads = keys.shape[1] // HD
    chunks = width // (key_heads * HD * HEADS)
    span = MAXSPAN * rows
    half = jnp.bfloat16
    dma = pltpu.SemaphoreType.DMA
    far_off = pl.BlockSpec(memory_space=pltpu.HBM)
    vmem = pl.BlockSpec(memory_space=pltpu.VMEM)
    small = (rows // recs, keys.shape[1])
    shapes = (
        jax.ShapeDtypeStruct(queries.shape, half),
        jax.ShapeDtypeStruct(small, half),
        jax.ShapeDtypeStruct(small, half),
    )
    grads = pl.pallas_call(
        kernel,
        out_shape=shapes,
        in_specs=[far_off] * 7,
        out_specs=(far_off, vmem, vmem),
        scratch_shapes=[
            pltpu.VMEM((rows, width), half),
            pltpu.VMEM((rows, width), half),
            pltpu.VMEM(log_sums.shape, jnp.float32),
            pltpu.VMEM(deltas.shape, jnp.float32),
            pltpu.SMEM(doc_ids.shape, jnp.int32),
            pltpu.VMEM((key_heads, 2, span, HD), half),
            pltpu.VMEM((key_heads, HD, span), half),
            pltpu.VMEM((span, width), half),
            pltpu.VMEM((rows, width), half),
            pltpu.VMEM((key_heads, 2, span, HD), jnp.float32),
            pltpu.VMEM((key_heads, BACK, 2, rows, HD), half),
            pltpu.VMEM((key_heads, BACK, 2, rows, HD), half),
            pltpu.VMEM((key_heads, 2, rows, HD), jnp.float32),
            pltpu.VMEM((key_heads, 2, rows, HD), half),
            pltpu.VMEM((key_heads, max(recs - 1, 1), 2, rows // recs, HD), half),
            dma((key_heads, chunks, 2)),
            dma((key_heads, 2)),
            dma((3,)),
            dma((key_heads, BACK)),
            dma((key_heads, BACK)),
            dma((key_heads, BACK)),
            dma((key_heads, BACK)),
            dma((key_heads, max(recs - 1, 1))),
            dma((key_heads, max(recs - 1, 1))),
            dma((key_heads, chunks)),
        ],
        compiler_params=pltpu.CompilerParams(
            collective_id=0, has_side_effects=True, vmem_limit_bytes=67_043_328
        ),
    )(queries, out_grads, log_sums, deltas, keys, values, doc_ids)
    return pl.pallas_call(
        finish,
        out_shape=shapes,
        in_specs=[far_off] * 3,
        out_specs=(far_off,) * 3,
        scratch_shapes=[
            pltpu.VMEM((PIECES, rows // PIECES, width), half),
            pltpu.VMEM(small, half),
            pltpu.VMEM(small, half),
            dma((PIECES + 2,)),
            dma((PIECES + 2,)),
        ],
        compiler_params=pltpu.CompilerParams(vmem_limit_bytes=67_043_328),
    )(*grads)


def solution(mesh):
    return jax.shard_map(
        per_device,
        mesh=mesh,
        in_specs=(
            P("rec", "ctx", None),
            P("rec", "ctx", None),
            P("rec", None, "ctx"),
            P("rec", None, "ctx"),
            P("ctx", None),
            P("ctx", None),
            P("rec", None),
        ),
        out_specs=(P("rec", "ctx", None), P(("ctx", "rec"), None), P(("ctx", "rec"), None)),
        check_vma=False,
    )
```

```python
import functools
import math

import jax
import jax.numpy as jnp
from jax import lax
from jax.experimental import pallas as pl
from jax.experimental.pallas import tpu as pltpu
from jax.sharding import PartitionSpec as P

HD = 128
MAXSPAN = 4
HEADS = 16
BACK = MAXSPAN - 1
MESH = pl.DeviceIdType.MESH
FAR = 1e30
PIECES = 4


def kernel(
    q_hbm, g_hbm, sums_hbm, delta_hbm, k_hbm, v_hbm, ids_hbm,
    dq_hbm, dk_ref, dv_ref,
    q_buf, g_buf, sums_ref, delta_ref, ids_ref, kv, key_t, ds_buf, dq_buf, acc, part, landed, total, r_send, r_land,
    load_sem, own_sem, small_sem, kv_send, kv_recv, g_send, g_recv, rec_send, rec_recv, out_sem,
):
    peers = lax.axis_size("ctx")
    recs = lax.axis_size("rec")
    mine = lax.axis_index("ctx")
    rec = lax.axis_index("rec")
    rows = q_buf.shape[0]
    key_heads = kv.shape[0]
    group = q_buf.shape[1] // (key_heads * HD)
    chunks = group // HEADS
    wide = HEADS * HD
    scale = HD ** (-0.5)
    fold = scale * math.log2(math.e)
    share = rows // recs

    def own_copy(g, which):
        source = (k_hbm, v_hbm)[which]
        return pltpu.make_async_copy(
            source.at[:, pl.ds(g * HD, HD)],
            kv.at[g, which, pl.ds(0, rows), :],
            own_sem.at[g, which],
        )

    def lanes(g, c):
        return pl.ds(pl.multiple_of((g * chunks + c) * wide, wide), wide)

    def load(g, c, which):
        source, target = ((q_hbm, q_buf), (g_hbm, g_buf))[which]
        return pltpu.make_async_copy(
            source.at[0, :, lanes(g, c)], target.at[:, lanes(g, c)], load_sem.at[g, c, which]
        )

    def out_copy(g, c):
        return pltpu.make_async_copy(
            dq_buf.at[:, lanes(g, c)], dq_hbm.at[0, :, lanes(g, c)], out_sem.at[g, c]
        )

    def kv_copy(g, k):
        return pltpu.make_async_remote_copy(
            src_ref=kv.at[g, :, pl.ds(0, rows), :],
            dst_ref=kv.at[g, :, pl.ds(k * rows, rows), :],
            send_sem=kv_send.at[g, k - 1],
            recv_sem=kv_recv.at[g, k - 1],
            device_id={"ctx": lax.rem(mine + k, peers)},
            device_id_type=MESH,
        )

    def grad_copy(g, k):
        return pltpu.make_async_remote_copy(
            src_ref=part.at[g, k - 1],
            dst_ref=landed.at[g, k - 1],
            send_sem=g_send.at[g, k - 1],
            recv_sem=g_recv.at[g, k - 1],
            device_id={"ctx": lax.rem(mine - k + peers, peers)},
            device_id_type=MESH,
        )

    def rec_copy(g, j):
        target = lax.rem(rec + j, recs)
        return pltpu.make_async_remote_copy(
            src_ref=r_send.at[g, :, pl.ds(pl.multiple_of(target * share, share), share), :],
            dst_ref=r_land.at[g, j - 1],
            send_sem=rec_send.at[g, j - 1],
            recv_sem=rec_recv.at[g, j - 1],
            device_id={"rec": target},
            device_id_type=MESH,
        )

    for g in range(key_heads):
        for which in range(2):
            own_copy(g, which).start()
    small = [
        pltpu.make_async_copy(source, target, small_sem.at[i])
        for i, (source, target) in enumerate(
            ((sums_hbm, sums_ref), (delta_hbm, delta_ref), (ids_hbm, ids_ref))
        )
    ]
    for copy in small:
        copy.start()
    for g in range(key_heads):
        for c in range(chunks):
            for which in range(2):
                load(g, c, which).start()

    barrier = pltpu.get_barrier_semaphore()
    for k in range(1, MAXSPAN):
        for other in (lax.rem(mine + k, peers), lax.rem(mine - k + peers, peers)):
            pl.semaphore_signal(barrier, inc=1, device_id={"ctx": other}, device_id_type=MESH)
    for j in range(1, recs):
        pl.semaphore_signal(
            barrier, inc=1, device_id={"rec": lax.rem(rec + j, recs)}, device_id_type=MESH
        )
    for k in range(1, MAXSPAN):
        @pl.when(mine < k)
        def _():
            kv[:, :, pl.ds(k * rows, rows), :] = jnp.zeros((key_heads, 2, rows, HD), kv.dtype)

        @pl.when(mine + k >= peers)
        def _():
            landed[:, k - 1] = jnp.zeros((key_heads, 2, rows, HD), landed.dtype)
    acc[...] = jnp.zeros_like(acc)
    pl.semaphore_wait(barrier, 2 * BACK + recs - 1)

    for g in range(key_heads):
        for which in range(2):
            own_copy(g, which).wait()
        for k in range(1, MAXSPAN):
            @pl.when(mine + k < peers)
            def _():
                kv_copy(g, k).start()

    for copy in small:
        copy.wait()
    here = ids_ref[0, mine]
    far = [jnp.float32(0.0)]
    for k in range(1, MAXSPAN):
        same = (ids_ref[0, jnp.maximum(mine - k, 0)] == here) & (mine >= k)
        far.append(jnp.where(same, 0.0, FAR).astype(jnp.float32))

    def heads_down(ref, g, c):
        first = (g * chunks + c) * HEADS
        return jnp.concatenate(
            [ref[:, pl.ds(pl.multiple_of((first + i) * HD, HD), HD)] for i in range(HEADS)], axis=0
        )

    def heads_along(ref, g, c):
        first = (g * chunks + c) * HEADS
        return jnp.concatenate([ref[0, pl.ds(first + i, 1), :] for i in range(HEADS)], axis=1)

    inner = (((1,), (1,)), ((), ()))

    def sweep(g, k):
        at = pl.ds(k * rows, rows)

        @pl.loop(0, chunks)
        def _(c):
            if k == 0:
                for which in range(2):
                    load(g, c, which).wait()
            query = heads_down(q_buf, g, c)
            grad = heads_down(g_buf, g, c)
            sums = heads_along(sums_ref, g, c) * math.log2(math.e) + far[k]
            delta = heads_along(delta_ref, g, c)
            scores = lax.dot_general(
                kv[g, 0, at, :], query, inner, preferred_element_type=jnp.float32
            )
            dprobs = lax.dot_general(
                kv[g, 1, at, :], grad, inner, preferred_element_type=jnp.float32
            )
            probs = jnp.exp2(scores * fold - sums)
            if k == 0:
                u = lax.broadcasted_iota(jnp.int32, (rows, wide), 0)
                t = lax.broadcasted_iota(jnp.int32, (rows, wide), 1) & (rows - 1)
                probs = jnp.where(u <= t, probs, 0.0)
            ds = (probs * (dprobs - delta)).astype(jnp.bfloat16)
            probs = probs.astype(jnp.bfloat16)
            ds_buf[at, lanes(g, c)] = ds
            acc[g, 0, at, :] += jnp.dot(ds, query, preferred_element_type=jnp.float32)
            acc[g, 1, at, :] += jnp.dot(probs, grad, preferred_element_type=jnp.float32)

    def query_side(g):
        @pl.loop(0, chunks)
        def _(c):
            dq = jnp.dot(
                key_t[g], ds_buf[:, lanes(g, c)], preferred_element_type=jnp.float32
            ) * scale
            for i in range(HEADS):
                at = pl.ds(pl.multiple_of(((g * chunks + c) * HEADS + i) * HD, HD), HD)
                dq_buf[:, at] = dq[:, i * rows:(i + 1) * rows].T.astype(dq_buf.dtype)
            out_copy(g, c).start()

    def turn(g, k):
        at = pl.ds(k * rows, rows)
        key_t[g, :, k * rows:(k + 1) * rows] = kv[g, 0, at, :].T

    def tile(g, k):
        @pl.when(mine >= k)
        def _():
            kv_copy(g, k).wait_recv()
        sweep(g, k)
        part[g, k - 1] = acc[g, :, k * rows:(k + 1) * rows, :].astype(part.dtype)

        @pl.when(mine >= k)
        def _():
            grad_copy(g, k).start()
        turn(g, k)

    def across(g):
        whole = acc[g, :, 0:rows, :]
        for k in range(1, MAXSPAN):
            @pl.when(mine + k < peers)
            def _():
                grad_copy(g, k).wait_recv()
        for k in range(1, MAXSPAN):
            whole = whole + landed[g, k - 1].astype(jnp.float32)
        total[g] = whole
        r_send[g] = whole.astype(r_send.dtype)
        for j in range(1, recs):
            rec_copy(g, j).start()

    def close(g):
        whole = total[g, :, pl.ds(pl.multiple_of(rec * share, share), share), :]
        for j in range(1, recs):
            rec_copy(g, j).wait_recv()
            whole = whole + r_land[g, j - 1].astype(jnp.float32)
        dk_ref[:, g * HD:(g + 1) * HD] = (whole[0] * scale).astype(dk_ref.dtype)
        dv_ref[:, g * HD:(g + 1) * HD] = whole[1].astype(dv_ref.dtype)

    last = key_heads - 1
    for g in range(key_heads):
        sweep(g, 0)
        turn(g, 0)
    for g in range(key_heads):
        order = range(1, MAXSPAN) if g < last else range(BACK, 0, -1)
        for k in order:
            tile(g, k)
    for g in range(last):
        across(g)
        query_side(g)
    across(last)
    query_side(last)
    for g in range(key_heads):
        close(g)
    for g in range(key_heads):
        for c in range(chunks):
            out_copy(g, c).wait()
        for k in range(1, MAXSPAN):
            @pl.when(mine + k < peers)
            def _():
                kv_copy(g, k).wait_send()

            @pl.when(mine >= k)
            def _():
                grad_copy(g, k).wait_send()
        for j in range(1, recs):
            rec_copy(g, j).wait_send()


def finish(dq_in, dk_in, dv_in, dq_out, dk_out, dv_out, big, dk, dv, into, out):
    pieces = big.shape[0]
    depth = big.shape[1]
    pairs = [
        (dq_in.at[0, pl.ds(i * depth, depth), :], big.at[i], dq_out.at[0, pl.ds(i * depth, depth), :])
        for i in range(pieces)
    ] + [(dk_in, dk, dk_out), (dv_in, dv, dv_out)]
    ins = [pltpu.make_async_copy(p[0], p[1], into.at[i]) for i, p in enumerate(pairs)]
    outs = [pltpu.make_async_copy(p[1], p[2], out.at[i]) for i, p in enumerate(pairs)]
    for copy in ins:
        copy.start()
    for arrived, leaving in zip(ins, outs):
        arrived.wait()
        leaving.start()
    for copy in outs:
        copy.wait()


def per_device(queries, out_grads, log_sums, deltas, keys, values, doc_ids):
    recs = lax.axis_size("rec")
    rows, width = queries.shape[1:]
    key_heads = keys.shape[1] // HD
    chunks = width // (key_heads * HD * HEADS)
    span = MAXSPAN * rows
    half = jnp.bfloat16
    dma = pltpu.SemaphoreType.DMA
    far_off = pl.BlockSpec(memory_space=pltpu.HBM)
    vmem = pl.BlockSpec(memory_space=pltpu.VMEM)
    small = (rows // recs, keys.shape[1])
    shapes = (
        jax.ShapeDtypeStruct(queries.shape, half),
        jax.ShapeDtypeStruct(small, half),
        jax.ShapeDtypeStruct(small, half),
    )
    grads = pl.pallas_call(
        kernel,
        out_shape=shapes,
        in_specs=[far_off] * 7,
        out_specs=(far_off, vmem, vmem),
        scratch_shapes=[
            pltpu.VMEM((rows, width), half),
            pltpu.VMEM((rows, width), half),
            pltpu.VMEM(log_sums.shape, jnp.float32),
            pltpu.VMEM(deltas.shape, jnp.float32),
            pltpu.SMEM(doc_ids.shape, jnp.int32),
            pltpu.VMEM((key_heads, 2, span, HD), half),
            pltpu.VMEM((key_heads, HD, span), half),
            pltpu.VMEM((span, width), half),
            pltpu.VMEM((rows, width), half),
            pltpu.VMEM((key_heads, 2, span, HD), jnp.float32),
            pltpu.VMEM((key_heads, BACK, 2, rows, HD), half),
            pltpu.VMEM((key_heads, BACK, 2, rows, HD), half),
            pltpu.VMEM((key_heads, 2, rows, HD), jnp.float32),
            pltpu.VMEM((key_heads, 2, rows, HD), half),
            pltpu.VMEM((key_heads, max(recs - 1, 1), 2, rows // recs, HD), half),
            dma((key_heads, chunks, 2)),
            dma((key_heads, 2)),
            dma((3,)),
            dma((key_heads, BACK)),
            dma((key_heads, BACK)),
            dma((key_heads, BACK)),
            dma((key_heads, BACK)),
            dma((key_heads, max(recs - 1, 1))),
            dma((key_heads, max(recs - 1, 1))),
            dma((key_heads, chunks)),
        ],
        compiler_params=pltpu.CompilerParams(
            collective_id=0, has_side_effects=True, vmem_limit_bytes=67_043_328
        ),
    )(queries, out_grads, log_sums, deltas, keys, values, doc_ids)
    return pl.pallas_call(
        finish,
        out_shape=shapes,
        in_specs=[far_off] * 3,
        out_specs=(far_off,) * 3,
        scratch_shapes=[
            pltpu.VMEM((PIECES, rows // PIECES, width), half),
            pltpu.VMEM(small, half),
            pltpu.VMEM(small, half),
            dma((PIECES + 2,)),
            dma((PIECES + 2,)),
        ],
        compiler_params=pltpu.CompilerParams(vmem_limit_bytes=67_043_328),
    )(*grads)


def solution(mesh):
    return jax.shard_map(
        per_device,
        mesh=mesh,
        in_specs=(
            P("rec", "ctx", None),
            P("rec", "ctx", None),
            P("rec", None, "ctx"),
            P("rec", None, "ctx"),
            P("ctx", None),
            P("ctx", None),
            P("rec", None),
        ),
        out_specs=(P("rec", "ctx", None), P(("ctx", "rec"), None), P(("ctx", "rec"), None)),
        check_vma=False,
    )
```
